32 devices in a mesh: role: 2 (over x), gy: 2 (over y), gx: 8 (over z, core).
Axes of the slice: x: 2, y: 2, z: 4, core: 2. Of those that a mesh axis runs over, the one named last changes fastest.
Arguments:
- thermal_anomaly: float32 [16, 192, 2048], P('role', 'gy', 'gx'), may hold values from -6 to 6
- saltiness_anomaly: float32 [16, 192, 2048], P('role', 'gy', 'gx'), may hold values from -6 to 6
- zonal_flow_fraction: bfloat16 [16, 192, 2048], P('role', 'gy', 'gx'), may hold values from -0.5 to 0.5
- meridional_flow_fraction: bfloat16 [16, 192, 2048], P('role', 'gy', 'gx'), may hold values from -0.5 to 0.5
- mixing_coefficient: float32 [16], P('role'), may hold values from 0.03 to 0.2
- continent_patch_numbering: int32 [2], replicated, may hold values from 0 to 15
- parallel_band_coefficients: bfloat16 [16, 4, 12], P('gy'), may hold values from -1.75 to 1.75
- meridian_panel_coefficients: bfloat16 [14, 512, 128], replicated, may hold values from -0.25 to 0.25
- panel_starting_source_meridian: int32 [14], replicated, may hold values from 0 to 1536, as said below
- target_parallel_cluster: int32 [64], replicated, may hold values from 0 to 7, as said below
Outputs:
- remapped: bfloat16 [3, 16, 64, 1792], P(None, 'role', ('gy', 'gx'))
- checksums: float32 [3, 8], replicated
The draws below stay inside these ranges and needn't reach their ends.
Inputs may be any that keep to these rules, and one draw needn't show every extreme that they name: `panel_starting_source_meridian`: every block's window lies within the model grid. `target_parallel_cluster`: each group number names exactly 8 rows.
All inputs are finite; a program needn't handle non-finite values.
Results may differ from the reference program's by a relative error of at most 0.0057.
Values may be sent and summed in bfloat16 or wider, within the bound.
A program may use at most 64 MiB of HBM per device.

```python
import math
import jax
import jax.numpy as jnp
from jax import lax

VERTICAL_LAYERS = 16
CY = 96
CX = 256
TR = 4
SW = 512
TB = 128
MESH_MERID_SIZE = 192
MESH_ZONAL_SIZE = 2048
NTILES = 16
NLAND = 2
NSTRIP = 16
SR = 12
NBLK = 14
NTX = 1792
NTY = 64
NGROUP = 8
N_GY = 2
N_GX = 8


def draw_panel_starting_source_meridian(key, part):
    starts = jax.random.randint(jax.random.fold_in(key, 3), (NBLK,), 0, MESH_ZONAL_SIZE - SW + 1)
    return starts.astype(jnp.int32)


def draw_target_parallel_cluster(key, part):
    order = jax.random.permutation(jax.random.fold_in(key, 7), NTY)
    return (order % NGROUP).astype(jnp.int32)


def steps_of(key, dims, cuts, least, top_value):
    def one(axis_at, parts):
        heights = jax.random.uniform(jax.random.fold_in(jax.random.fold_in(key, 6), axis_at), (parts,), jnp.float32, least / len(cuts), top_value / len(cuts))
        return jnp.repeat(jnp.exp(heights), dims[axis_at] // parts).reshape((-1,) + (1,) * (len(dims) - axis_at - 1))

    level = one(*cuts[0])
    for cut in cuts[1:]:
        level = level * one(*cut)
    return level


def gaussian(key, extent, spread, limit, pieces=(), kind=jnp.bfloat16):
    array = spread * jax.random.normal(key, extent, jnp.float32)
    if pieces:
        array = array * steps_of(key, extent, pieces, -0.22, 0.18)
    return jnp.clip(array, -limit, limit).astype(kind)


def setup_inputs(seed: int = 0) -> dict:
    streams_of = jax.random.split(jax.random.key(seed), 11)
    return {
        "thermal_anomaly": gaussian(streams_of[0], (VERTICAL_LAYERS, MESH_MERID_SIZE, MESH_ZONAL_SIZE), 1.0, 6.0, ((0, 2), (1, 2), (2, 8)), jnp.float32),
        "saltiness_anomaly": gaussian(streams_of[1], (VERTICAL_LAYERS, MESH_MERID_SIZE, MESH_ZONAL_SIZE), 1.0, 6.0, ((0, 2), (1, 2), (2, 8)), jnp.float32),
        "zonal_flow_fraction": jnp.clip(jax.random.uniform(streams_of[2], (VERTICAL_LAYERS, MESH_MERID_SIZE, MESH_ZONAL_SIZE), jnp.float32, -0.5, 0.5) * steps_of(streams_of[2], (VERTICAL_LAYERS, MESH_MERID_SIZE, MESH_ZONAL_SIZE), ((0, 2), (1, 2), (2, 8)), -0.4, 0.0), -0.5, 0.5).astype(jnp.bfloat16),
        "meridional_flow_fraction": jnp.clip(jax.random.uniform(streams_of[3], (VERTICAL_LAYERS, MESH_MERID_SIZE, MESH_ZONAL_SIZE), jnp.float32, -0.5, 0.5) * steps_of(streams_of[3], (VERTICAL_LAYERS, MESH_MERID_SIZE, MESH_ZONAL_SIZE), ((0, 2), (1, 2), (2, 8)), -0.4, 0.0), -0.5, 0.5).astype(jnp.bfloat16),
        "mixing_coefficient": jnp.clip(jnp.exp(math.log(0.2) - 1.89712 * jax.random.uniform(streams_of[4], (VERTICAL_LAYERS,), jnp.float32) ** steps_of(streams_of[4], (VERTICAL_LAYERS,), ((0, 2),), -0.2, 0.2)), 0.03, 0.2),
        "continent_patch_numbering": jax.random.randint(streams_of[5], (NLAND,), 0, NTILES).astype(jnp.int32),
        "parallel_band_coefficients": gaussian(streams_of[6], (NSTRIP, TR, SR), SR ** -0.5, 1.75, ((0, 2),)),
        "meridian_panel_coefficients": gaussian(streams_of[7], (NBLK, SW, TB), SW ** -0.5, 0.25),
        "panel_starting_source_meridian": draw_panel_starting_source_meridian(jax.random.fold_in(streams_of[10], 71), 0),
        "target_parallel_cluster": draw_target_parallel_cluster(jax.random.fold_in(streams_of[10], 71), 0),
    }


def step_level(tracers, east_speed, north_speed, kappa, ocean):
    padded = jnp.pad(tracers, ((0, 0), (1, 1), (0, 0)))
    east = jnp.roll(tracers, -1, axis=2)
    west = jnp.roll(tracers, 1, axis=2)
    north = padded[:, 2:, :]
    south = padded[:, :-2, :]
    tendency = -east_speed * (east - west) * 0.5 - north_speed * (north - south) * 0.5 + kappa * (east + west + north + south - 4.0 * tracers)
    return tracers + ocean * tendency


def density(temp, salt, level):
    return 0.78 * salt - 0.17 * temp * (1.0 + 0.03 * level) - 0.02 * temp * temp


def reference(thermal_anomaly, saltiness_anomaly, zonal_flow_fraction, meridional_flow_fraction, mixing_coefficient, continent_patch_numbering, parallel_band_coefficients, meridian_panel_coefficients, panel_starting_source_meridian, target_parallel_cluster):
    tiles = N_GY * N_GX
    listed = jnp.any(continent_patch_numbering[:, None] == jnp.arange(tiles, dtype=jnp.int32)[None, :], axis=0)
    flags = 1.0 - listed.astype(jnp.float32)
    ocean = jnp.repeat(jnp.repeat(flags.reshape(N_GY, N_GX), CY, axis=0), CX, axis=1)
    lat_f = parallel_band_coefficients.astype(jnp.float32)
    lon_f = meridian_panel_coefficients.astype(jnp.float32)
    vertical_layer_total = jnp.arange(VERTICAL_LAYERS, dtype=jnp.float32)

    def lone_vertical_layer(packed):
        temp, salt, east_raw, north_raw, kappa, level = packed
        east_speed = east_raw.astype(jnp.float32)
        north_speed = north_raw.astype(jnp.float32)
        scalar_field_pair = jnp.stack([temp, salt])
        means = jnp.zeros((3, MESH_MERID_SIZE, MESH_ZONAL_SIZE), jnp.float32)
        for step in range(2):
            scalar_field_pair = step_level(scalar_field_pair, east_speed, north_speed, kappa, ocean)
            rho = density(scalar_field_pair[0], scalar_field_pair[1], level)
            means = means + jnp.stack([scalar_field_pair[0], scalar_field_pair[1], rho])
        means = (0.5 * means).astype(jnp.bfloat16)
        strips = means.astype(jnp.float32).reshape(3, NSTRIP, SR, MESH_ZONAL_SIZE)
        lat_out = jnp.einsum("gts,fgsx->fgtx", lat_f, strips, precision=lax.Precision.HIGHEST)
        lat_out = lat_out.astype(jnp.bfloat16).reshape(3, NTY, MESH_ZONAL_SIZE)

        def block(index):
            window = lax.dynamic_slice_in_dim(lat_out, panel_starting_source_meridian[index].astype(jnp.int32), SW, axis=2)
            return jnp.einsum("frs,st->frt", window.astype(jnp.float32), lon_f[index], precision=lax.Precision.HIGHEST)

        blocks = lax.map(block, jnp.arange(NBLK, dtype=jnp.int32))
        values = jnp.transpose(blocks, (1, 2, 0, 3)).reshape(3, NTY, NBLK * TB)
        quadratic_entries = jnp.sum(values * values, axis=2)
        return values.astype(jnp.bfloat16), quadratic_entries

    regridded_target_field, quadratic_entries = lax.map(lone_vertical_layer, (thermal_anomaly, saltiness_anomaly, zonal_flow_fraction, meridional_flow_fraction, mixing_coefficient, vertical_layer_total))
    remapped = jnp.transpose(regridded_target_field, (1, 0, 2, 3))
    thick = 1.0 + 0.25 * vertical_layer_total
    rows = jnp.arange(NTY, dtype=jnp.float32)
    area = jnp.cos((-75.0 + 150.0 * (rows + 0.5) / NTY) * (math.pi / 180.0))
    weighted = jnp.sum(quadratic_entries * thick[:, None, None], axis=0) * area[None, :]
    onehot = (target_parallel_cluster[:, None] == jnp.arange(NGROUP, dtype=jnp.int32)[None, :]).astype(jnp.float32)
    numer = jnp.dot(weighted, onehot, precision=lax.Precision.HIGHEST)
    denom = jnp.sum(thick) * NTX * jnp.dot(area, onehot, precision=lax.Precision.HIGHEST)
    return remapped, numer / denom[None, :]
```

```python
import functools
import math

import jax
import jax.numpy as jnp
import numpy as np
from jax import lax
from jax.experimental import pallas as pl
from jax.experimental.pallas import tpu as pltpu
from jax.sharding import PartitionSpec as P

LANES = 128
F32 = jnp.float32
BF16 = jnp.bfloat16
MESH = pl.DeviceIdType.MESH


def wrap(value, count):
    return jnp.where(value >= count, value - count, value)


def iota(shape, dim):
    return lax.broadcasted_iota(jnp.int32, shape, dim)


def peer_of(dims, d):
    n_role, n_gy, n_gx = dims[:3]
    role, gy, gx = (lax.axis_index(a) for a in ("role", "gy", "gx"))
    dx, dyr = d % n_gx, d // n_gx
    dy, dr = dyr % n_gy, dyr // n_gy
    return (wrap(role + dr, n_role), wrap(gy + dy, n_gy), wrap(gx + dx, n_gx))


def model_kernel(
    dims,
    temp_hbm,
    salt_hbm,
    zonal_hbm,
    merid_hbm,
    kappa_ref,
    land_ref,
    band_ref,
    lat_out,
    x0,
    x1,
    zonal,
    merid,
    band_rows,
    means,
    lat_send,
    lat_recv,
    row_send,
    row_recv,
    col_send,
    col_recv,
    in_sems,
    halo_send_sems,
    halo_recv_sems,
    a2a_send_sems,
    a2a_recv_sems,
    local_sems,
):
    n_role, n_gy, n_gx, levels, cy, cx, trows, srows, nblk, sw, tb, groups = dims
    role, gy, gx = (lax.axis_index(a) for a in ("role", "gy", "gx"))
    lev_grp = 16 // trows
    halves = levels // lev_grp

    loads = [
        pltpu.make_async_copy(temp_hbm, x0.at[0], in_sems.at[0]),
        pltpu.make_async_copy(salt_hbm, x0.at[1], in_sems.at[1]),
        pltpu.make_async_copy(zonal_hbm, zonal, in_sems.at[2]),
        pltpu.make_async_copy(merid_hbm, merid, in_sems.at[3]),
    ]
    for load in loads:
        load.start()

    peer = functools.partial(peer_of, dims)
    barrier = pltpu.get_barrier_semaphore()
    greeted = [d for d in range(1, n_gx)] + [d * n_gx for d in range(1, n_role * n_gy)]
    for d in greeted:
        pl.semaphore_signal(barrier, inc=1, device_id=peer(d), device_id_type=MESH)

    band_rows[...] = jnp.zeros_like(band_rows)

    lane = iota((cy, LANES), 1)

    def pack_columns(s, tiles):
        first = jnp.zeros((cy, LANES), F32)
        last = jnp.zeros((cy, LANES), F32)
        for t in range(2):
            for l in range(levels):
                k = t * levels + l
                head = tiles[t, l, :, pl.ds(0, LANES)]
                tail = tiles[t, l, :, pl.ds(cx - LANES, LANES)]
                first = jnp.where(lane == k, pltpu.roll(head, k, 1) if k else head, first)
                last = jnp.where(lane == k, pltpu.roll(tail, k + 1, 1), last)
        col_send[s, 0] = first
        col_send[s, 1] = last

    def pack_rows(s, t, l, head, tail):
        row_send[s, 0, t, pl.ds(l, 1), :] = head
        row_send[s, 1, t, pl.ds(l, 1), :] = tail

    west = wrap(gx + n_gx - 1, n_gx)
    east = wrap(gx + 1, n_gx)
    below = wrap(gy + n_gy - 1, n_gy)
    above = wrap(gy + 1, n_gy)

    def halo_copies(s):
        copies = []
        for i, (send, recv, d, target) in enumerate(
            (
                (col_send, col_recv, 0, (role, gy, west)),
                (col_send, col_recv, 1, (role, gy, east)),
                (row_send, row_recv, 0, (role, below, gx)),
                (row_send, row_recv, 1, (role, above, gx)),
            )
        ):
            copies.append(
                pltpu.make_async_remote_copy(
                    src_ref=send.at[s, d],
                    dst_ref=recv.at[s, d],
                    send_sem=halo_send_sems.at[s, i],
                    recv_sem=halo_recv_sems.at[s, i],
                    device_id=target,
                    device_id_type=MESH,
                )
            )
        return copies

    loads[0].wait()
    loads[1].wait()
    for t in range(2):
        for l in range(levels):
            pack_rows(0, t, l, x0[t, l, pl.ds(0, 1), :], x0[t, l, pl.ds(cy - 1, 1), :])
    pack_columns(0, x0)
    pl.semaphore_wait(barrier, len(greeted))
    halo0 = halo_copies(0)
    for copy in halo0:
        copy.start()

    for g in range(n_gx):
        band_rows[pl.ds(g * trows, trows), pl.ds(0, srows)] = band_ref[g].astype(F32)
    brows = band_rows.shape[0]
    out_r, in_r = n_gx * lev_grp * trows, lev_grp * cy
    ri, rq = iota((out_r, brows), 0), iota((out_r, brows), 1)
    pick_r = (lax.div(ri, lev_grp * trows) == lax.div(rq, trows)) & (
        lax.rem(ri, trows) == lax.rem(rq, trows)
    )
    spread = jnp.dot(
        pick_r.astype(F32).astype(BF16), band_rows[...].astype(BF16), preferred_element_type=F32
    )
    cs, cc = iota((LANES, in_r), 0), iota((LANES, in_r), 1)
    pick_c = lax.rem(lax.rem(cc, cy), srows) == cs
    spread = jnp.dot(
        spread.astype(BF16), pick_c.astype(F32).astype(BF16), preferred_element_type=F32
    )
    ai, ac = iota((out_r, in_r), 0), iota((out_r, in_r), 1)
    keep = (lax.div(lax.rem(ai, lev_grp * trows), trows) == lax.div(ac, cy)) & (
        lax.div(lax.rem(ac, cy), srows) == lax.div(ai, lev_grp * trows)
    )
    band = jnp.where(keep, spread, 0.0).astype(BF16)

    number = gy * n_gx + gx
    ocean = jnp.ones((1, cx), F32)
    for i in range(land_ref.shape[0]):
        ocean = jnp.where(jnp.full((1, cx), land_ref[i], jnp.int32) == number, 0.0, ocean)

    wide = iota((cy, cx), 1)
    tall = iota((cy, cx), 0)
    has_above = jnp.where(gy < n_gy - 1, 1.0, 0.0).astype(F32)
    has_below = jnp.where(gy > 0, 1.0, 0.0).astype(F32)

    def advance(s, tiles, l):
        u = zonal[l].astype(F32) * (0.5 * ocean)
        v = merid[l].astype(F32) * (0.5 * ocean)
        kap = kappa_ref[l] * ocean
        own = 1.0 - 4.0 * kap
        results = []
        for t in range(2):
            k = t * levels + l
            c = tiles[t, l]
            e = jnp.where(
                wide == cx - 1, col_recv[s, 0, :, pl.ds(k, 1)], pltpu.roll(c, cx - 1, 1)
            )
            w = jnp.where(wide == 0, col_recv[s, 1, :, pl.ds(k, 1)], pltpu.roll(c, 1, 1))
            n = jnp.where(
                tall == cy - 1,
                row_recv[s, 0, t, pl.ds(l, 1), :] * has_above,
                pltpu.roll(c, cy - 1, 0),
            )
            b = jnp.where(
                tall == 0, row_recv[s, 1, t, pl.ds(l, 1), :] * has_below, pltpu.roll(c, 1, 0)
            )
            results.append(
                own * c + (kap * (e + w + n + b) - u * (e - w) - v * (n - b))
            )
        return results

    loads[2].wait()
    loads[3].wait()
    for copy in halo0:
        copy.wait()
    for l in range(levels):
        new = advance(0, x0, l)
        for t in range(2):
            x1[t, l] = new[t]
            pack_rows(1, t, l, new[t][:1], new[t][cy - 1 :])
    pack_columns(1, x1)
    halo1 = halo_copies(1)
    for copy in halo1:
        copy.start()

    for copy in halo1:
        copy.wait()

    mine = pl.multiple_of(gx * cx, LANES)
    exchanges = []
    local = []
    for h in range(halves):
        for l in range(h * lev_grp, (h + 1) * lev_grp):
            new = advance(1, x1, l)
            lev = (role * levels + l).astype(F32)
            factor = 0.17 * (1.0 + 0.03 * lev)
            t1, s1 = x1[0, l], x1[1, l]
            t2, s2 = new
            r1 = 0.78 * s1 - factor * t1 - 0.02 * t1 * t1
            r2 = 0.78 * s2 - factor * t2 - 0.02 * t2 * t2
            means[0, l] = (0.5 * (t1 + t2)).astype(BF16)
            means[1, l] = (0.5 * (s1 + s2)).astype(BF16)
            means[2, l] = (0.5 * (r1 + r2)).astype(BF16)
        for f in range(3):
            rows = means[f, pl.ds(h * lev_grp, lev_grp)].reshape(in_r, cx)
            lat = jnp.dot(band, rows, preferred_element_type=F32).astype(BF16)
            for g in range(n_gx):
                lat_send[g, f, h] = lat[g * 16 : (g + 1) * 16]
        for d in range(1, n_gx):
            target = wrap(gx + d, n_gx)
            copy = pltpu.make_async_remote_copy(
                src_ref=lat_send.at[target, :, h],
                dst_ref=lat_recv.at[:, h, :, pl.ds(mine, cx)],
                send_sem=a2a_send_sems.at[h, d],
                recv_sem=a2a_recv_sems.at[h, d],
                device_id=(role, gy, target),
                device_id_type=MESH,
            )
            copy.start()
            exchanges.append((h, copy))
        copy = pltpu.make_async_copy(
            lat_send.at[gx, :, h], lat_recv.at[:, h, :, pl.ds(mine, cx)], local_sems.at[h]
        )
        copy.start()
        local.append(copy)

    for _, copy in exchanges:
        copy.wait()
    for copy in local:
        copy.wait()
    lat_out[:, :, :, pl.ds(0, n_gx * cx)] = lat_recv[...]
    lat_out[:, :, :, pl.ds(n_gx * cx, LANES)] = jnp.zeros(lat_out.shape[:3] + (LANES,), BF16)


def remap_kernel(
    dims, lat_ref, panel_hbm, start_ref, cluster_ref, area_ref, out_ref, part_ref, panel, pad, sems
):
    n_role, n_gy, n_gx, levels, cy, cx, trows, srows, nblk, sw, tb, groups = dims
    role, gy, gx = (lax.axis_index(a) for a in ("role", "gy", "gx"))
    loads = [
        pltpu.make_async_copy(panel_hbm.at[j], panel.at[j], sems.at[j]) for j in range(nblk)
    ]
    for load in loads:
        load.start()
    pad[:, pl.ds(0, LANES), :] = jnp.zeros((nblk, LANES, tb), F32)
    pad[:, pl.ds(LANES + sw, LANES), :] = jnp.zeros((nblk, LANES, tb), F32)

    glanes = part_ref.shape[1]
    labels = iota((1, glanes), 1)

    def add_area(r, so_far):
        return so_far + jnp.where(labels == cluster_ref[r], area_ref[r], 0.0)

    zero = jnp.zeros((1, glanes), F32)
    all_rows = cluster_ref.shape[0]
    area_sum = lax.fori_loop(0, all_rows, add_area, zero, unroll=8)
    thick_total = sum(1.0 + 0.25 * k for k in range(levels * n_role))
    denom = area_sum * (thick_total * nblk * tb)

    first_row = (gy * n_gx + gx) * trows
    out_rows = 3 * levels * trows
    row = iota((out_rows, 1), 0)
    ti = lax.rem(row, trows)
    hot = jnp.zeros((out_rows, glanes), F32)
    for t in range(trows):
        row_hot = jnp.where(labels == cluster_ref[first_row + t], area_ref[first_row + t], 0.0)
        hot = jnp.where(ti == t, row_hot, hot)
    level = role * levels + lax.rem(lax.div(row, trows), levels)
    thick = 1.0 + 0.25 * level.astype(F32)

    squares = jnp.zeros((out_rows, tb), F32)
    for j in range(nblk):
        start = start_ref[j]
        base = lax.div(start, LANES) * LANES
        loads[j].wait()
        pad[j, pl.ds(LANES, sw), :] = panel[j].astype(F32)
        weights = pad[j, pl.ds(LANES - (start - base), sw + LANES), :].astype(BF16)
        window = lat_ref[:, pl.ds(pl.multiple_of(base, LANES), sw + LANES)]
        values = jnp.dot(window, weights, preferred_element_type=F32)
        squares = squares + values * values
        out_ref[:, pl.ds(j * tb, tb)] = values.astype(BF16)
    weighted = jnp.sum(squares, axis=1, keepdims=True) * thick * hot
    part_ref[...] = jnp.zeros_like(part_ref)
    named = labels < groups
    for f in range(3):
        size = levels * trows
        numer = jnp.sum(weighted[f * size : (f + 1) * size], axis=0, keepdims=True)
        part_ref[pl.ds(f, 1), :] = jnp.where(named, numer / jnp.where(named, denom, 1.0), 0.0)


def sums_kernel(dims, part_ref, sums_ref, gather, sum_sems):
    n_role, n_gy, n_gx = dims[:3]
    groups = dims[-1]
    role, gy, gx = (lax.axis_index(a) for a in ("role", "gy", "gx"))
    total = n_role * n_gy * n_gx
    me = (role * n_gy + gy) * n_gx + gx
    barrier = pltpu.get_barrier_semaphore()

    def for_others(do):
        if total <= 64:
            for d in range(1, total):
                do(peer_of(dims, d))
        else:

            @pl.loop(1, total)
            def _(d):
                do(peer_of(dims, d))

    def greet(device):
        pl.semaphore_signal(barrier, inc=1, device_id=device, device_id_type=MESH)

    def send(device):
        pltpu.make_async_remote_copy(
            src_ref=gather.at[me],
            dst_ref=gather.at[me],
            send_sem=sum_sems.at[0],
            recv_sem=sum_sems.at[1],
            device_id=device,
            device_id_type=MESH,
        ).start()

    for_others(greet)
    gather[me] = part_ref[...]
    pl.semaphore_wait(barrier, total - 1)
    for_others(send)
    every = gather.at[pl.ds(0, total - 1)]
    for i in (1, 0):
        pltpu.make_async_copy(every, every, sum_sems.at[i]).wait()
    sums_ref[...] = jnp.sum(gather[...], axis=0)[:3, :groups]


def body(
    dims,
    area,
    thermal_anomaly,
    saltiness_anomaly,
    zonal_flow_fraction,
    meridional_flow_fraction,
    mixing_coefficient,
    continent_patch_numbering,
    parallel_band_coefficients,
    meridian_panel_coefficients,
    panel_starting_source_meridian,
    target_parallel_cluster,
):
    n_role, n_gy, n_gx, levels, cy, cx, trows, srows, nblk, sw, tb, groups = dims
    total = n_role * n_gy * n_gx
    lev_grp = 16 // trows
    halves = levels // lev_grp
    glanes = -(-groups // LANES) * LANES
    hbm = pl.BlockSpec(memory_space=pl.ANY)
    smem = pl.BlockSpec(memory_space=pltpu.SMEM)
    vmem = pl.BlockSpec(memory_space=pltpu.VMEM)
    brows = -(-n_gx * trows // LANES) * LANES
    dma = pltpu.SemaphoreType.DMA
    mib = 1024 * 1024
    lat = pl.pallas_call(
        functools.partial(model_kernel, dims),
        out_shape=jax.ShapeDtypeStruct((3, halves, 16, n_gx * cx + LANES), BF16),
        in_specs=[hbm] * 4 + [smem, smem, vmem],
        out_specs=vmem,
        scratch_shapes=[
            pltpu.VMEM((2, levels, cy, cx), F32),
            pltpu.VMEM((2, levels, cy, cx), F32),
            pltpu.VMEM((levels, cy, cx), BF16),
            pltpu.VMEM((levels, cy, cx), BF16),
            pltpu.VMEM((brows, LANES), F32),
            pltpu.VMEM((3, levels, cy, cx), BF16),
            pltpu.VMEM((n_gx, 3, halves, 16, cx), BF16),
            pltpu.VMEM((3, halves, 16, n_gx * cx), BF16),
            pltpu.VMEM((2, 2, 2, levels, cx), F32),
            pltpu.VMEM((2, 2, 2, levels, cx), F32),
            pltpu.VMEM((2, 2, cy, LANES), F32),
            pltpu.VMEM((2, 2, cy, LANES), F32),
            dma((4,)),
            dma((2, 4)),
            dma((2, 4)),
            dma((halves, n_gx)),
            dma((halves, n_gx)),
            dma((halves,)),
        ],
        compiler_params=pltpu.CompilerParams(
            collective_id=0, has_side_effects=True, vmem_limit_bytes=20 * mib
        ),
        name="model",
    )(
        thermal_anomaly,
        saltiness_anomaly,
        zonal_flow_fraction,
        meridional_flow_fraction,
        mixing_coefficient,
        continent_patch_numbering,
        parallel_band_coefficients,
    )
    out_rows = 3 * levels * trows
    remapped, part = pl.pallas_call(
        functools.partial(remap_kernel, dims),
        out_shape=(
            jax.ShapeDtypeStruct((out_rows, nblk * tb), BF16),
            jax.ShapeDtypeStruct((8, glanes), F32),
        ),
        in_specs=[vmem, hbm, smem, smem, smem],
        out_specs=(vmem, vmem),
        scratch_shapes=[
            pltpu.VMEM((nblk, sw, tb), BF16),
            pltpu.VMEM((nblk, sw + 2 * LANES, tb), F32),
            dma((nblk,)),
        ],
        compiler_params=pltpu.CompilerParams(vmem_limit_bytes=30 * mib),
        name="remap",
    )(
        lat.reshape(out_rows, n_gx * cx + LANES),
        meridian_panel_coefficients,
        panel_starting_source_meridian,
        target_parallel_cluster,
        jnp.asarray(area),
    )
    sums = pl.pallas_call(
        functools.partial(sums_kernel, dims),
        out_shape=jax.ShapeDtypeStruct((3, groups), F32),
        in_specs=[vmem],
        out_specs=vmem,
        scratch_shapes=[pltpu.VMEM((total, 8, glanes), F32), dma((2,))],
        compiler_params=pltpu.CompilerParams(
            collective_id=1, has_side_effects=True, vmem_limit_bytes=16 * mib
        ),
        name="sums",
    )(part)
    return remapped.reshape(3, levels, trows, nblk * tb), sums


def solution(mesh):
    in_specs = (
        P("role", "gy", "gx"),
        P("role", "gy", "gx"),
        P("role", "gy", "gx"),
        P("role", "gy", "gx"),
        P("role"),
        P(),
        P("gy", None, None),
        P(),
        P(),
        P(),
    )
    out_specs = (P(None, "role", ("gy", "gx"), None), P())

    def run(*args):
        n_role, n_gy, n_gx = (mesh.shape[a] for a in ("role", "gy", "gx"))
        levels, rows, cols = args[0].shape
        _, trows, srows = args[6].shape
        nblk, sw, tb = args[7].shape
        dims = (
            n_role,
            n_gy,
            n_gx,
            levels // n_role,
            rows // n_gy,
            cols // n_gx,
            trows,
            srows,
            nblk,
            sw,
            tb,
            4 * n_gy,
        )
        nrows = args[9].shape[0]
        r = np.arange(nrows, dtype=np.float64)
        area = np.cos((-75.0 + 150.0 * (r + 0.5) / nrows) * (math.pi / 180.0)).astype(np.float32)
        return jax.shard_map(
            functools.partial(body, dims, area),
            mesh=mesh,
            in_specs=in_specs,
            out_specs=out_specs,
            check_vma=False,
        )(*args)

    return run
```

```python
import functools
import math

import jax
import jax.numpy as jnp
import numpy as np
from jax import lax
from jax.experimental import pallas as pl
from jax.experimental.pallas import tpu as pltpu
from jax.sharding import PartitionSpec as P

LANES = 128
F32 = jnp.float32
BF16 = jnp.bfloat16
MESH = pl.DeviceIdType.MESH


def wrap(value, count):
    return jnp.where(value >= count, value - count, value)


def iota(shape, dim):
    return lax.broadcasted_iota(jnp.int32, shape, dim)


def peer_of(dims, d):
    n_role, n_gy, n_gx = dims[:3]
    role, gy, gx = (lax.axis_index(a) for a in ("role", "gy", "gx"))
    dx, dyr = d % n_gx, d // n_gx
    dy, dr = dyr % n_gy, dyr // n_gy
    return (wrap(role + dr, n_role), wrap(gy + dy, n_gy), wrap(gx + dx, n_gx))


def model_kernel(
    dims,
    temp_hbm,
    salt_hbm,
    zonal_hbm,
    merid_hbm,
    kappa_ref,
    land_ref,
    band_ref,
    lat_out,
    x0,
    x1,
    zonal,
    merid,
    band_rows,
    means,
    lat_send,
    lat_recv,
    row_send,
    row_recv,
    col_send,
    col_recv,
    in_sems,
    halo_send_sems,
    halo_recv_sems,
    a2a_send_sems,
    a2a_recv_sems,
    local_sems,
    out_sems,
):
    n_role, n_gy, n_gx, levels, cy, cx, trows, srows, nblk, sw, tb, groups = dims
    role, gy, gx = (lax.axis_index(a) for a in ("role", "gy", "gx"))
    lev_grp = 16 // trows
    halves = levels // lev_grp

    loads = [
        pltpu.make_async_copy(temp_hbm, x0.at[0], in_sems.at[0]),
        pltpu.make_async_copy(salt_hbm, x0.at[1], in_sems.at[1]),
        pltpu.make_async_copy(zonal_hbm, zonal, in_sems.at[2]),
        pltpu.make_async_copy(merid_hbm, merid, in_sems.at[3]),
    ]
    for load in loads:
        load.start()

    peer = functools.partial(peer_of, dims)
    barrier = pltpu.get_barrier_semaphore()
    greeted = [d for d in range(1, n_gx)] + [d * n_gx for d in range(1, n_role * n_gy)]
    for d in greeted:
        pl.semaphore_signal(barrier, inc=1, device_id=peer(d), device_id_type=MESH)

    band_rows[...] = jnp.zeros_like(band_rows)

    lane = iota((cy, LANES), 1)

    def pack_columns(s, tiles):
        first = jnp.zeros((cy, LANES), F32)
        last = jnp.zeros((cy, LANES), F32)
        for t in range(2):
            for l in range(levels):
                k = t * levels + l
                head = tiles[t, l, :, pl.ds(0, LANES)]
                tail = tiles[t, l, :, pl.ds(cx - LANES, LANES)]
                first = jnp.where(lane == k, pltpu.roll(head, k, 1) if k else head, first)
                last = jnp.where(lane == k, pltpu.roll(tail, k + 1, 1), last)
        col_send[s, 0] = first
        col_send[s, 1] = last

    def pack_rows(s, t, l, head, tail):
        row_send[s, 0, t, pl.ds(l, 1), :] = head
        row_send[s, 1, t, pl.ds(l, 1), :] = tail

    west = wrap(gx + n_gx - 1, n_gx)
    east = wrap(gx + 1, n_gx)
    below = wrap(gy + n_gy - 1, n_gy)
    above = wrap(gy + 1, n_gy)

    def halo_copies(s):
        copies = []
        for i, (send, recv, d, target) in enumerate(
            (
                (col_send, col_recv, 0, (role, gy, west)),
                (col_send, col_recv, 1, (role, gy, east)),
                (row_send, row_recv, 0, (role, below, gx)),
                (row_send, row_recv, 1, (role, above, gx)),
            )
        ):
            copies.append(
                pltpu.make_async_remote_copy(
                    src_ref=send.at[s, d],
                    dst_ref=recv.at[s, d],
                    send_sem=halo_send_sems.at[s, i],
                    recv_sem=halo_recv_sems.at[s, i],
                    device_id=target,
                    device_id_type=MESH,
                )
            )
        return copies

    loads[0].wait()
    loads[1].wait()
    for t in range(2):
        for l in range(levels):
            pack_rows(0, t, l, x0[t, l, pl.ds(0, 1), :], x0[t, l, pl.ds(cy - 1, 1), :])
    pack_columns(0, x0)
    pl.semaphore_wait(barrier, len(greeted))
    halo0 = halo_copies(0)
    for copy in halo0:
        copy.start()

    for g in range(n_gx):
        band_rows[pl.ds(g * trows, trows), pl.ds(0, srows)] = band_ref[g].astype(F32)
    brows = band_rows.shape[0]
    out_r, in_r = n_gx * lev_grp * trows, lev_grp * cy
    ri, rq = iota((out_r, brows), 0), iota((out_r, brows), 1)
    pick_r = (lax.div(ri, lev_grp * trows) == lax.div(rq, trows)) & (
        lax.rem(ri, trows) == lax.rem(rq, trows)
    )
    spread = jnp.dot(
        pick_r.astype(F32).astype(BF16), band_rows[...].astype(BF16), preferred_element_type=F32
    )
    cs, cc = iota((LANES, in_r), 0), iota((LANES, in_r), 1)
    pick_c = lax.rem(lax.rem(cc, cy), srows) == cs
    spread = jnp.dot(
        spread.astype(BF16), pick_c.astype(F32).astype(BF16), preferred_element_type=F32
    )
    ai, ac = iota((out_r, in_r), 0), iota((out_r, in_r), 1)
    keep = (lax.div(lax.rem(ai, lev_grp * trows), trows) == lax.div(ac, cy)) & (
        lax.div(lax.rem(ac, cy), srows) == lax.div(ai, lev_grp * trows)
    )
    band = jnp.where(keep, spread, 0.0).astype(BF16)

    number = gy * n_gx + gx
    ocean = jnp.ones((1, cx), F32)
    for i in range(land_ref.shape[0]):
        ocean = jnp.where(jnp.full((1, cx), land_ref[i], jnp.int32) == number, 0.0, ocean)

    wide = iota((cy, cx), 1)
    tall = iota((cy, cx), 0)
    has_above = jnp.where(gy < n_gy - 1, 1.0, 0.0).astype(F32)
    has_below = jnp.where(gy > 0, 1.0, 0.0).astype(F32)

    def advance(s, tiles, l):
        u = zonal[l].astype(F32) * (0.5 * ocean)
        v = merid[l].astype(F32) * (0.5 * ocean)
        kap = kappa_ref[l] * ocean
        own = 1.0 - 4.0 * kap
        results = []
        for t in range(2):
            k = t * levels + l
            c = tiles[t, l]
            e = jnp.where(
                wide == cx - 1, col_recv[s, 0, :, pl.ds(k, 1)], pltpu.roll(c, cx - 1, 1)
            )
            w = jnp.where(wide == 0, col_recv[s, 1, :, pl.ds(k, 1)], pltpu.roll(c, 1, 1))
            n = jnp.where(
                tall == cy - 1,
                row_recv[s, 0, t, pl.ds(l, 1), :] * has_above,
                pltpu.roll(c, cy - 1, 0),
            )
            b = jnp.where(
                tall == 0, row_recv[s, 1, t, pl.ds(l, 1), :] * has_below, pltpu.roll(c, 1, 0)
            )
            results.append(
                own * c + (kap * (e + w + n + b) - u * (e - w) - v * (n - b))
            )
        return results

    loads[2].wait()
    loads[3].wait()
    for copy in halo0:
        copy.wait()
    for l in range(levels):
        new = advance(0, x0, l)
        for t in range(2):
            x1[t, l] = new[t]
            pack_rows(1, t, l, new[t][:1], new[t][cy - 1 :])
    pack_columns(1, x1)
    halo1 = halo_copies(1)
    for copy in halo1:
        copy.start()

    for copy in halo1:
        copy.wait()

    mine = pl.multiple_of(gx * cx, LANES)
    exchanges = []
    local = []
    for h in range(halves):
        for l in range(h * lev_grp, (h + 1) * lev_grp):
            new = advance(1, x1, l)
            lev = (role * levels + l).astype(F32)
            factor = 0.17 * (1.0 + 0.03 * lev)
            t1, s1 = x1[0, l], x1[1, l]
            t2, s2 = new
            r1 = 0.78 * s1 - factor * t1 - 0.02 * t1 * t1
            r2 = 0.78 * s2 - factor * t2 - 0.02 * t2 * t2
            means[0, l] = (0.5 * (t1 + t2)).astype(BF16)
            means[1, l] = (0.5 * (s1 + s2)).astype(BF16)
            means[2, l] = (0.5 * (r1 + r2)).astype(BF16)
        for f in range(3):
            rows = means[f, pl.ds(h * lev_grp, lev_grp)].reshape(in_r, cx)
            lat = jnp.dot(band, rows, preferred_element_type=F32).astype(BF16)
            for g in range(n_gx):
                lat_send[g, f, h] = lat[g * 16 : (g + 1) * 16]
        for d in range(1, n_gx):
            target = wrap(gx + d, n_gx)
            copy = pltpu.make_async_remote_copy(
                src_ref=lat_send.at[target, :, h],
                dst_ref=lat_recv.at[:, h, :, pl.ds(mine, cx)],
                send_sem=a2a_send_sems.at[h, d],
                recv_sem=a2a_recv_sems.at[h, d],
                device_id=(role, gy, target),
                device_id_type=MESH,
            )
            copy.start()
            exchanges.append((h, copy))
        copy = pltpu.make_async_copy(
            lat_send.at[gx, :, h], lat_recv.at[:, h, :, pl.ds(mine, cx)], local_sems.at[h]
        )
        copy.start()
        local.append(copy)

    stores = []
    for h in range(halves):
        for when, copy in exchanges:
            if when == h:
                copy.wait_recv()
        local[h].wait()
        store = pltpu.make_async_copy(lat_recv.at[:, h], lat_out.at[:, h], out_sems.at[h])
        store.start()
        stores.append(store)
    for _, copy in exchanges:
        copy.wait_send()
    for store in stores:
        store.wait()


def remap_kernel(
    dims,
    lat_hbm,
    panel_hbm,
    start_ref,
    cluster_ref,
    area_ref,
    out_ref,
    part_ref,
    lat,
    wide,
    panel,
    sems,
):
    n_role, n_gy, n_gx, levels, cy, cx, trows, srows, nblk, sw, tb, groups = dims
    role, gy, gx = (lax.axis_index(a) for a in ("role", "gy", "gx"))
    lat_load = pltpu.make_async_copy(lat_hbm, lat, sems.at[nblk])
    lat_load.start()
    loads = [
        pltpu.make_async_copy(panel_hbm.at[j], panel.at[j], sems.at[j]) for j in range(nblk)
    ]
    for load in loads:
        load.start()

    glanes = part_ref.shape[1]
    lanes = iota((1, glanes), 1)
    labels = lax.rem(lanes, groups)

    def add_area(r, so_far):
        return so_far + jnp.where(labels == cluster_ref[r], area_ref[r], 0.0)

    zero = jnp.zeros((1, glanes), F32)
    all_rows = cluster_ref.shape[0]
    area_sum = lax.fori_loop(0, all_rows, add_area, zero, unroll=8)
    thick_total = sum(1.0 + 0.25 * k for k in range(levels * n_role))
    denom = area_sum * (thick_total * nblk * tb)

    first_row = (gy * n_gx + gx) * trows
    out_rows = 3 * levels * trows
    row = iota((out_rows, 1), 0)
    ti = lax.rem(row, trows)
    hot = jnp.zeros((out_rows, glanes), F32)
    for t in range(trows):
        row_hot = jnp.where(labels == cluster_ref[first_row + t], area_ref[first_row + t], 0.0)
        hot = jnp.where(ti == t, row_hot, hot)
    level = role * levels + lax.rem(lax.div(row, trows), levels)
    thick = 1.0 + 0.25 * level.astype(F32)

    lat_load.wait()
    columns = n_gx * cx
    wide[:, pl.ds(0, columns)] = lat[...].astype(F32)
    wide[:, pl.ds(columns, LANES)] = jnp.zeros((out_rows, LANES), F32)
    lane = iota((out_rows, LANES), 1)
    squares = jnp.zeros((out_rows, tb), F32)
    for j in range(nblk):
        start = start_ref[j]
        base = lax.div(start, LANES) * LANES
        shift = LANES - (start - base)
        turned = []
        for i in range(sw // LANES + 1):
            tile = wide[:, pl.ds(pl.multiple_of(base + i * LANES, LANES), LANES)]
            turned.append(pltpu.roll(tile, lax.rem(shift, LANES), 1))
        window = jnp.concatenate(
            [
                jnp.where(lane < shift, turned[i], turned[i + 1]).astype(BF16)
                for i in range(sw // LANES)
            ],
            axis=1,
        )
        loads[j].wait()
        values = jnp.dot(window, panel[j], preferred_element_type=F32)
        squares = squares + values * values
        out_ref[:, pl.ds(j * tb, tb)] = values.astype(BF16)
    weighted = jnp.sum(squares, axis=1, keepdims=True) * thick * hot
    size = levels * trows
    field = lax.div(lanes, groups)
    numer = jnp.zeros((1, glanes), F32)
    for f in range(3):
        own = jnp.sum(weighted[f * size : (f + 1) * size], axis=0, keepdims=True)
        numer = jnp.where(field == f, own, numer)
    part_ref[...] = numer / denom


def sums_kernel(dims, part_ref, sums_ref, gather, sum_sems):
    n_role, n_gy, n_gx = dims[:3]
    role, gy, gx = (lax.axis_index(a) for a in ("role", "gy", "gx"))
    total = n_role * n_gy * n_gx
    me = (role * n_gy + gy) * n_gx + gx
    barrier = pltpu.get_barrier_semaphore()

    def for_others(do):
        if total <= 64:
            for d in range(1, total):
                do(peer_of(dims, d))
        else:

            @pl.loop(1, total)
            def _(d):
                do(peer_of(dims, d))

    def greet(device):
        pl.semaphore_signal(barrier, inc=1, device_id=device, device_id_type=MESH)

    def send(device):
        pltpu.make_async_remote_copy(
            src_ref=gather.at[me],
            dst_ref=gather.at[me],
            send_sem=sum_sems.at[0],
            recv_sem=sum_sems.at[1],
            device_id=device,
            device_id_type=MESH,
        ).start()

    for_others(greet)
    gather[me] = part_ref[...]
    pl.semaphore_wait(barrier, total - 1)
    for_others(send)
    every = gather.at[pl.ds(0, total - 1)]
    for i in (1, 0):
        pltpu.make_async_copy(every, every, sum_sems.at[i]).wait()
    sums_ref[...] = jnp.sum(gather[...], axis=0)


def body(
    dims,
    area,
    thermal_anomaly,
    saltiness_anomaly,
    zonal_flow_fraction,
    meridional_flow_fraction,
    mixing_coefficient,
    continent_patch_numbering,
    parallel_band_coefficients,
    meridian_panel_coefficients,
    panel_starting_source_meridian,
    target_parallel_cluster,
):
    n_role, n_gy, n_gx, levels, cy, cx, trows, srows, nblk, sw, tb, groups = dims
    total = n_role * n_gy * n_gx
    lev_grp = 16 // trows
    halves = levels // lev_grp
    glanes = -(-3 * groups // LANES) * LANES
    hbm = pl.BlockSpec(memory_space=pl.ANY)
    smem = pl.BlockSpec(memory_space=pltpu.SMEM)
    vmem = pl.BlockSpec(memory_space=pltpu.VMEM)
    brows = -(-n_gx * trows // LANES) * LANES
    dma = pltpu.SemaphoreType.DMA
    mib = 1024 * 1024
    lat = pl.pallas_call(
        functools.partial(model_kernel, dims),
        out_shape=jax.ShapeDtypeStruct((3, halves, 16, n_gx * cx), BF16),
        in_specs=[hbm] * 4 + [smem, smem, vmem],
        out_specs=hbm,
        scratch_shapes=[
            pltpu.VMEM((2, levels, cy, cx), F32),
            pltpu.VMEM((2, levels, cy, cx), F32),
            pltpu.VMEM((levels, cy, cx), BF16),
            pltpu.VMEM((levels, cy, cx), BF16),
            pltpu.VMEM((brows, LANES), F32),
            pltpu.VMEM((3, levels, cy, cx), BF16),
            pltpu.VMEM((n_gx, 3, halves, 16, cx), BF16),
            pltpu.VMEM((3, halves, 16, n_gx * cx), BF16),
            pltpu.VMEM((2, 2, 2, levels, cx), F32),
            pltpu.VMEM((2, 2, 2, levels, cx), F32),
            pltpu.VMEM((2, 2, cy, LANES), F32),
            pltpu.VMEM((2, 2, cy, LANES), F32),
            dma((4,)),
            dma((2, 4)),
            dma((2, 4)),
            dma((halves, n_gx)),
            dma((halves, n_gx)),
            dma((halves,)),
            dma((halves,)),
        ],
        compiler_params=pltpu.CompilerParams(
            collective_id=0, has_side_effects=True, vmem_limit_bytes=60 * mib
        ),
        name="model",
    )(
        thermal_anomaly,
        saltiness_anomaly,
        zonal_flow_fraction,
        meridional_flow_fraction,
        mixing_coefficient,
        continent_patch_numbering,
        parallel_band_coefficients,
    )
    out_rows = 3 * levels * trows
    remapped, part = pl.pallas_call(
        functools.partial(remap_kernel, dims),
        out_shape=(
            jax.ShapeDtypeStruct((out_rows, nblk * tb), BF16),
            jax.ShapeDtypeStruct((1, glanes), F32),
        ),
        in_specs=[hbm, hbm, smem, smem, smem],
        out_specs=(vmem, vmem),
        scratch_shapes=[
            pltpu.VMEM((out_rows, n_gx * cx), BF16),
            pltpu.VMEM((out_rows, n_gx * cx + LANES), F32),
            pltpu.VMEM((nblk, sw, tb), BF16),
            dma((nblk + 1,)),
        ],
        compiler_params=pltpu.CompilerParams(vmem_limit_bytes=60 * mib),
        name="remap",
    )(
        lat.reshape(out_rows, n_gx * cx),
        meridian_panel_coefficients,
        panel_starting_source_meridian,
        target_parallel_cluster,
        jnp.asarray(area),
    )
    sums = pl.pallas_call(
        functools.partial(sums_kernel, dims),
        out_shape=jax.ShapeDtypeStruct((1, glanes), F32),
        in_specs=[vmem],
        out_specs=vmem,
        scratch_shapes=[pltpu.VMEM((total, 1, glanes), F32), dma((2,))],
        compiler_params=pltpu.CompilerParams(
            collective_id=1, has_side_effects=True, vmem_limit_bytes=16 * mib
        ),
        name="sums",
    )(part)
    return remapped.reshape(3, levels, trows, nblk * tb), sums[0, : 3 * groups].reshape(3, groups)


def solution(mesh):
    in_specs = (
        P("role", "gy", "gx"),
        P("role", "gy", "gx"),
        P("role", "gy", "gx"),
        P("role", "gy", "gx"),
        P("role"),
        P(),
        P("gy", None, None),
        P(),
        P(),
        P(),
    )
    out_specs = (P(None, "role", ("gy", "gx"), None), P())

    def run(*args):
        n_role, n_gy, n_gx = (mesh.shape[a] for a in ("role", "gy", "gx"))
        levels, rows, cols = args[0].shape
        _, trows, srows = args[6].shape
        nblk, sw, tb = args[7].shape
        dims = (
            n_role,
            n_gy,
            n_gx,
            levels // n_role,
            rows // n_gy,
            cols // n_gx,
            trows,
            srows,
            nblk,
            sw,
            tb,
            4 * n_gy,
        )
        nrows = args[9].shape[0]
        r = np.arange(nrows, dtype=np.float64)
        area = np.cos((-75.0 + 150.0 * (r + 0.5) / nrows) * (math.pi / 180.0)).astype(np.float32)
        return jax.shard_map(
            functools.partial(body, dims, area),
            mesh=mesh,
            in_specs=in_specs,
            out_specs=out_specs,
            check_vma=False,
        )(*args)

    return run
```

```python
import functools
import math

import jax
import jax.numpy as jnp
import numpy as np
from jax import lax
from jax.experimental import pallas as pl
from jax.experimental.pallas import tpu as pltpu
from jax.sharding import PartitionSpec as P

LANES = 128
F32 = jnp.float32
BF16 = jnp.bfloat16
MESH = pl.DeviceIdType.MESH


def wrap(value, count):
    return jnp.where(value >= count, value - count, value)


def iota(shape, dim):
    return lax.broadcasted_iota(jnp.int32, shape, dim)


def peer_of(dims, d):
    n_role, n_gy, n_gx = dims[:3]
    role, gy, gx = (lax.axis_index(a) for a in ("role", "gy", "gx"))
    dx, dyr = d % n_gx, d // n_gx
    dy, dr = dyr % n_gy, dyr // n_gy
    return (wrap(role + dr, n_role), wrap(gy + dy, n_gy), wrap(gx + dx, n_gx))


def model_kernel(
    dims,
    temp_hbm,
    salt_hbm,
    zonal_hbm,
    merid_hbm,
    kappa_ref,
    land_ref,
    band_ref,
    lat_out,
    x0,
    x1,
    zonal,
    merid,
    band_rows,
    means,
    lat_send,
    lat_recv,
    row_send,
    row_recv,
    col_send,
    col_recv,
    in_sems,
    halo_send_sems,
    halo_recv_sems,
    a2a_send_sems,
    a2a_recv_sems,
    local_sems,
    out_sems,
):
    n_role, n_gy, n_gx, levels, cy, cx, trows, srows, nblk, sw, tb, groups = dims
    role, gy, gx = (lax.axis_index(a) for a in ("role", "gy", "gx"))
    lev_grp = 16 // trows
    halves = levels // lev_grp

    loads = [
        pltpu.make_async_copy(temp_hbm, x0.at[0], in_sems.at[0]),
        pltpu.make_async_copy(salt_hbm, x0.at[1], in_sems.at[1]),
        pltpu.make_async_copy(zonal_hbm, zonal, in_sems.at[2]),
        pltpu.make_async_copy(merid_hbm, merid, in_sems.at[3]),
    ]
    for load in loads:
        load.start()

    peer = functools.partial(peer_of, dims)
    barrier = pltpu.get_barrier_semaphore()
    greeted = [d for d in range(1, n_gx)] + [d * n_gx for d in range(1, n_role * n_gy)]
    for d in greeted:
        pl.semaphore_signal(barrier, inc=1, device_id=peer(d), device_id_type=MESH)

    band_rows[...] = jnp.zeros_like(band_rows)

    lane = iota((cy, LANES), 1)

    def pack_columns(s, tiles):
        first = jnp.zeros((cy, LANES), F32)
        last = jnp.zeros((cy, LANES), F32)
        for t in range(2):
            for l in range(levels):
                k = t * levels + l
                head = tiles[t, l, :, pl.ds(0, LANES)]
                tail = tiles[t, l, :, pl.ds(cx - LANES, LANES)]
                first = jnp.where(lane == k, pltpu.roll(head, k, 1) if k else head, first)
                last = jnp.where(lane == k, pltpu.roll(tail, k + 1, 1), last)
        col_send[s, 0] = first
        col_send[s, 1] = last

    def pack_rows(s, t, l, head, tail):
        row_send[s, 0, t, pl.ds(l, 1), :] = head
        row_send[s, 1, t, pl.ds(l, 1), :] = tail

    west = wrap(gx + n_gx - 1, n_gx)
    east = wrap(gx + 1, n_gx)
    below = wrap(gy + n_gy - 1, n_gy)
    above = wrap(gy + 1, n_gy)

    def halo_copies(s):
        copies = []
        for i, (send, recv, d, target) in enumerate(
            (
                (col_send, col_recv, 0, (role, gy, west)),
                (col_send, col_recv, 1, (role, gy, east)),
                (row_send, row_recv, 0, (role, below, gx)),
                (row_send, row_recv, 1, (role, above, gx)),
            )
        ):
            copies.append(
                pltpu.make_async_remote_copy(
                    src_ref=send.at[s, d],
                    dst_ref=recv.at[s, d],
                    send_sem=halo_send_sems.at[s, i],
                    recv_sem=halo_recv_sems.at[s, i],
                    device_id=target,
                    device_id_type=MESH,
                )
            )
        return copies

    loads[0].wait()
    loads[1].wait()
    for t in range(2):
        for l in range(levels):
            pack_rows(0, t, l, x0[t, l, pl.ds(0, 1), :], x0[t, l, pl.ds(cy - 1, 1), :])
    pack_columns(0, x0)
    pl.semaphore_wait(barrier, len(greeted))
    halo0 = halo_copies(0)
    for copy in halo0:
        copy.start()

    for g in range(n_gx):
        band_rows[pl.ds(g * trows, trows), pl.ds(0, srows)] = band_ref[g].astype(F32)
    brows = band_rows.shape[0]
    out_r, in_r = n_gx * lev_grp * trows, lev_grp * cy
    ri, rq = iota((out_r, brows), 0), iota((out_r, brows), 1)
    pick_r = (lax.div(ri, lev_grp * trows) == lax.div(rq, trows)) & (
        lax.rem(ri, trows) == lax.rem(rq, trows)
    )
    spread = jnp.dot(
        pick_r.astype(F32).astype(BF16), band_rows[...].astype(BF16), preferred_element_type=F32
    )
    cs, cc = iota((LANES, in_r), 0), iota((LANES, in_r), 1)
    pick_c = lax.rem(lax.rem(cc, cy), srows) == cs
    spread = jnp.dot(
        spread.astype(BF16), pick_c.astype(F32).astype(BF16), preferred_element_type=F32
    )
    ai, ac = iota((out_r, in_r), 0), iota((out_r, in_r), 1)
    keep = (lax.div(lax.rem(ai, lev_grp * trows), trows) == lax.div(ac, cy)) & (
        lax.div(lax.rem(ac, cy), srows) == lax.div(ai, lev_grp * trows)
    )
    band = jnp.where(keep, spread, 0.0).astype(BF16)

    number = gy * n_gx + gx
    ocean = jnp.ones((1, cx), F32)
    for i in range(land_ref.shape[0]):
        ocean = jnp.where(jnp.full((1, cx), land_ref[i], jnp.int32) == number, 0.0, ocean)

    wide = iota((cy, cx), 1)
    tall = iota((cy, cx), 0)
    has_above = jnp.where(gy < n_gy - 1, 1.0, 0.0).astype(F32)
    has_below = jnp.where(gy > 0, 1.0, 0.0).astype(F32)

    def advance(s, tiles, l):
        u = zonal[l].astype(F32) * (0.5 * ocean)
        v = merid[l].astype(F32) * (0.5 * ocean)
        kap = kappa_ref[l] * ocean
        own = 1.0 - 4.0 * kap
        results = []
        for t in range(2):
            k = t * levels + l
            c = tiles[t, l]
            e = jnp.where(
                wide == cx - 1, col_recv[s, 0, :, pl.ds(k, 1)], pltpu.roll(c, cx - 1, 1)
            )
            w = jnp.where(wide == 0, col_recv[s, 1, :, pl.ds(k, 1)], pltpu.roll(c, 1, 1))
            n = jnp.where(
                tall == cy - 1,
                row_recv[s, 0, t, pl.ds(l, 1), :] * has_above,
                pltpu.roll(c, cy - 1, 0),
            )
            b = jnp.where(
                tall == 0, row_recv[s, 1, t, pl.ds(l, 1), :] * has_below, pltpu.roll(c, 1, 0)
            )
            results.append(
                own * c + (kap * (e + w + n + b) - u * (e - w) - v * (n - b))
            )
        return results

    loads[2].wait()
    loads[3].wait()
    for copy in halo0:
        copy.wait()
    for l in range(levels):
        new = advance(0, x0, l)
        for t in range(2):
            x1[t, l] = new[t]
            pack_rows(1, t, l, new[t][:1], new[t][cy - 1 :])
    pack_columns(1, x1)
    halo1 = halo_copies(1)
    for copy in halo1:
        copy.start()

    for copy in halo1:
        copy.wait()

    mine = pl.multiple_of(gx * cx, LANES)
    exchanges = []
    local = []
    for h in range(halves):
        for l in range(h * lev_grp, (h + 1) * lev_grp):
            new = advance(1, x1, l)
            lev = (role * levels + l).astype(F32)
            factor = 0.17 * (1.0 + 0.03 * lev)
            t1, s1 = x1[0, l], x1[1, l]
            t2, s2 = new
            r1 = 0.78 * s1 - factor * t1 - 0.02 * t1 * t1
            r2 = 0.78 * s2 - factor * t2 - 0.02 * t2 * t2
            means[0, l] = (0.5 * (t1 + t2)).astype(BF16)
            means[1, l] = (0.5 * (s1 + s2)).astype(BF16)
            means[2, l] = (0.5 * (r1 + r2)).astype(BF16)
        for f in range(3):
            rows = means[f, pl.ds(h * lev_grp, lev_grp)].reshape(in_r, cx)
            lat = jnp.dot(band, rows, preferred_element_type=F32).astype(BF16)
            for g in range(n_gx):
                lat_send[g, f, h] = lat[g * 16 : (g + 1) * 16]
        for d in range(1, n_gx):
            target = wrap(gx + d, n_gx)
            copy = pltpu.make_async_remote_copy(
                src_ref=lat_send.at[target, :, h],
                dst_ref=lat_recv.at[:, h, :, pl.ds(mine, cx)],
                send_sem=a2a_send_sems.at[h, d],
                recv_sem=a2a_recv_sems.at[h, d],
                device_id=(role, gy, target),
                device_id_type=MESH,
            )
            copy.start()
            exchanges.append((h, copy))
        copy = pltpu.make_async_copy(
            lat_send.at[gx, :, h], lat_recv.at[:, h, :, pl.ds(mine, cx)], local_sems.at[h]
        )
        copy.start()
        local.append(copy)

    stores = []
    for h in range(halves):
        for when, copy in exchanges:
            if when == h:
                copy.wait_recv()
        local[h].wait()
        store = pltpu.make_async_copy(lat_recv.at[:, h], lat_out.at[:, h], out_sems.at[h])
        store.start()
        stores.append(store)
    for _, copy in exchanges:
        copy.wait_send()
    for store in stores:
        store.wait()


def remap_kernel(
    dims,
    lat_hbm,
    panel_hbm,
    start_ref,
    cluster_ref,
    area_ref,
    out_ref,
    part_ref,
    lat,
    wide,
    result,
    panel,
    sems,
):
    n_role, n_gy, n_gx, levels, cy, cx, trows, srows, nblk, sw, tb, groups = dims
    role, gy, gx = (lax.axis_index(a) for a in ("role", "gy", "gx"))
    lat_load = pltpu.make_async_copy(lat_hbm, lat, sems.at[nblk])
    lat_load.start()
    loads = [
        pltpu.make_async_copy(panel_hbm.at[j], panel.at[j], sems.at[j]) for j in range(nblk)
    ]
    for load in loads:
        load.start()

    glanes = part_ref.shape[1]
    lanes = iota((1, glanes), 1)
    labels = lax.rem(lanes, groups)

    def add_area(r, so_far):
        return so_far + jnp.where(labels == cluster_ref[r], area_ref[r], 0.0)

    zero = jnp.zeros((1, glanes), F32)
    all_rows = cluster_ref.shape[0]
    area_sum = lax.fori_loop(0, all_rows, add_area, zero, unroll=8)
    thick_total = sum(1.0 + 0.25 * k for k in range(levels * n_role))
    denom = area_sum * (thick_total * nblk * tb)

    first_row = (gy * n_gx + gx) * trows
    out_rows = 3 * levels * trows
    row = iota((out_rows, 1), 0)
    ti = lax.rem(row, trows)
    hot = jnp.zeros((out_rows, glanes), F32)
    for t in range(trows):
        row_hot = jnp.where(labels == cluster_ref[first_row + t], area_ref[first_row + t], 0.0)
        hot = jnp.where(ti == t, row_hot, hot)
    level = role * levels + lax.rem(lax.div(row, trows), levels)
    thick = 1.0 + 0.25 * level.astype(F32)

    lat_load.wait()
    columns = n_gx * cx
    wide[:, pl.ds(0, columns)] = lat[...].astype(F32)
    wide[:, pl.ds(columns, LANES)] = jnp.zeros((out_rows, LANES), F32)
    lane = iota((out_rows, LANES), 1)
    squares = jnp.zeros((out_rows, tb), F32)
    for j in range(nblk):
        start = start_ref[j]
        base = lax.div(start, LANES) * LANES
        shift = LANES - (start - base)
        turned = []
        for i in range(sw // LANES + 1):
            tile = wide[:, pl.ds(pl.multiple_of(base + i * LANES, LANES), LANES)]
            turned.append(pltpu.roll(tile, lax.rem(shift, LANES), 1))
        window = jnp.concatenate(
            [
                jnp.where(lane < shift, turned[i], turned[i + 1]).astype(BF16)
                for i in range(sw // LANES)
            ],
            axis=1,
        )
        loads[j].wait()
        values = jnp.dot(window, panel[j], preferred_element_type=F32)
        squares = squares + values * values
        result[:, pl.ds(j * tb, tb)] = values
    for i in range(3 * levels):
        out_ref[i // levels, i % levels] = result[pl.ds(i * trows, trows), :].astype(BF16)
    weighted = jnp.sum(squares, axis=1, keepdims=True) * thick * hot
    size = levels * trows
    field = lax.div(lanes, groups)
    numer = jnp.zeros((1, glanes), F32)
    for f in range(3):
        own = jnp.sum(weighted[f * size : (f + 1) * size], axis=0, keepdims=True)
        numer = jnp.where(field == f, own, numer)
    part_ref[...] = numer / denom


def sums_kernel(dims, part_ref, sums_ref, gather, sum_sems):
    n_role, n_gy, n_gx = dims[:3]
    role, gy, gx = (lax.axis_index(a) for a in ("role", "gy", "gx"))
    total = n_role * n_gy * n_gx
    me = (role * n_gy + gy) * n_gx + gx
    barrier = pltpu.get_barrier_semaphore()

    def for_others(do):
        if total <= 64:
            for d in range(1, total):
                do(peer_of(dims, d))
        else:

            @pl.loop(1, total)
            def _(d):
                do(peer_of(dims, d))

    def greet(device):
        pl.semaphore_signal(barrier, inc=1, device_id=device, device_id_type=MESH)

    def send(device):
        pltpu.make_async_remote_copy(
            src_ref=gather.at[me],
            dst_ref=gather.at[me],
            send_sem=sum_sems.at[0],
            recv_sem=sum_sems.at[1],
            device_id=device,
            device_id_type=MESH,
        ).start()

    for_others(greet)
    gather[me] = part_ref[...]
    pl.semaphore_wait(barrier, total - 1)
    for_others(send)
    every = gather.at[pl.ds(0, total - 1)]
    for i in (1, 0):
        pltpu.make_async_copy(every, every, sum_sems.at[i]).wait()
    sums_ref[...] = jnp.sum(gather[...], axis=0)


def body(
    dims,
    area,
    thermal_anomaly,
    saltiness_anomaly,
    zonal_flow_fraction,
    meridional_flow_fraction,
    mixing_coefficient,
    continent_patch_numbering,
    parallel_band_coefficients,
    meridian_panel_coefficients,
    panel_starting_source_meridian,
    target_parallel_cluster,
):
    n_role, n_gy, n_gx, levels, cy, cx, trows, srows, nblk, sw, tb, groups = dims
    total = n_role * n_gy * n_gx
    lev_grp = 16 // trows
    halves = levels // lev_grp
    glanes = -(-3 * groups // LANES) * LANES
    hbm = pl.BlockSpec(memory_space=pl.ANY)
    smem = pl.BlockSpec(memory_space=pltpu.SMEM)
    vmem = pl.BlockSpec(memory_space=pltpu.VMEM)
    brows = -(-n_gx * trows // LANES) * LANES
    dma = pltpu.SemaphoreType.DMA
    mib = 1024 * 1024
    lat = pl.pallas_call(
        functools.partial(model_kernel, dims),
        out_shape=jax.ShapeDtypeStruct((3, halves, 16, n_gx * cx), BF16),
        in_specs=[hbm] * 4 + [smem, smem, vmem],
        out_specs=hbm,
        scratch_shapes=[
            pltpu.VMEM((2, levels, cy, cx), F32),
            pltpu.VMEM((2, levels, cy, cx), F32),
            pltpu.VMEM((levels, cy, cx), BF16),
            pltpu.VMEM((levels, cy, cx), BF16),
            pltpu.VMEM((brows, LANES), F32),
            pltpu.VMEM((3, levels, cy, cx), BF16),
            pltpu.VMEM((n_gx, 3, halves, 16, cx), BF16),
            pltpu.VMEM((3, halves, 16, n_gx * cx), BF16),
            pltpu.VMEM((2, 2, 2, levels, cx), F32),
            pltpu.VMEM((2, 2, 2, levels, cx), F32),
            pltpu.VMEM((2, 2, cy, LANES), F32),
            pltpu.VMEM((2, 2, cy, LANES), F32),
            dma((4,)),
            dma((2, 4)),
            dma((2, 4)),
            dma((halves, n_gx)),
            dma((halves, n_gx)),
            dma((halves,)),
            dma((halves,)),
        ],
        compiler_params=pltpu.CompilerParams(
            collective_id=0, has_side_effects=True, vmem_limit_bytes=60 * mib
        ),
        name="model",
    )(
        thermal_anomaly,
        saltiness_anomaly,
        zonal_flow_fraction,
        meridional_flow_fraction,
        mixing_coefficient,
        continent_patch_numbering,
        parallel_band_coefficients,
    )
    out_rows = 3 * levels * trows
    remapped, part = pl.pallas_call(
        functools.partial(remap_kernel, dims),
        out_shape=(
            jax.ShapeDtypeStruct((3, levels, trows, nblk * tb), BF16),
            jax.ShapeDtypeStruct((1, glanes), F32),
        ),
        in_specs=[hbm, hbm, smem, smem, smem],
        out_specs=(vmem, vmem),
        scratch_shapes=[
            pltpu.VMEM((out_rows, n_gx * cx), BF16),
            pltpu.VMEM((out_rows, n_gx * cx + LANES), F32),
            pltpu.VMEM((out_rows, nblk * tb), F32),
            pltpu.VMEM((nblk, sw, tb), BF16),
            dma((nblk + 1,)),
        ],
        compiler_params=pltpu.CompilerParams(vmem_limit_bytes=60 * mib),
        name="remap",
    )(
        lat.reshape(out_rows, n_gx * cx),
        meridian_panel_coefficients,
        panel_starting_source_meridian,
        target_parallel_cluster,
        jnp.asarray(area),
    )
    sums = pl.pallas_call(
        functools.partial(sums_kernel, dims),
        out_shape=jax.ShapeDtypeStruct((1, glanes), F32),
        in_specs=[vmem],
        out_specs=vmem,
        scratch_shapes=[pltpu.VMEM((total, 1, glanes), F32), dma((2,))],
        compiler_params=pltpu.CompilerParams(
            collective_id=1, has_side_effects=True, vmem_limit_bytes=16 * mib
        ),
        name="sums",
    )(part)
    return remapped, sums[0, : 3 * groups].reshape(3, groups)


def solution(mesh):
    in_specs = (
        P("role", "gy", "gx"),
        P("role", "gy", "gx"),
        P("role", "gy", "gx"),
        P("role", "gy", "gx"),
        P("role"),
        P(),
        P("gy", None, None),
        P(),
        P(),
        P(),
    )
    out_specs = (P(None, "role", ("gy", "gx"), None), P())

    def run(*args):
        n_role, n_gy, n_gx = (mesh.shape[a] for a in ("role", "gy", "gx"))
        levels, rows, cols = args[0].shape
        _, trows, srows = args[6].shape
        nblk, sw, tb = args[7].shape
        dims = (
            n_role,
            n_gy,
            n_gx,
            levels // n_role,
            rows // n_gy,
            cols // n_gx,
            trows,
            srows,
            nblk,
            sw,
            tb,
            4 * n_gy,
        )
        nrows = args[9].shape[0]
        r = np.arange(nrows, dtype=np.float64)
        area = np.cos((-75.0 + 150.0 * (r + 0.5) / nrows) * (math.pi / 180.0)).astype(np.float32)
        return jax.shard_map(
            functools.partial(body, dims, area),
            mesh=mesh,
            in_specs=in_specs,
            out_specs=out_specs,
            check_vma=False,
        )(*args)

    return run
```
